32 devices in a mesh: rep: 8 (over y, x, core), tp: 4 (over z).
Axes of the slice: x: 2, y: 2, z: 4, core: 2. Of those that a mesh axis runs over, the one named last changes fastest.
Arguments:
- flat_buffer: bfloat16 [578912256], P(('rep', 'tp')), may hold values from -60 to 60
- shard_pad: int32 [2, 6], replicated, may hold values from 0 to 2
Outputs:
- q_served: bfloat16 [2, 6144, 6144], P(None, 'rep', 'tp')
- q_scale: float32 [2, 48, 6144], P(None, 'rep', 'tp')
- k_served: bfloat16 [2, 6144, 1024], P(None, 'rep', 'tp')
- k_scale: float32 [2, 48, 1024], P(None, 'rep', 'tp')
- v_served: bfloat16 [2, 6144, 1024], P(None, 'rep', 'tp')
- v_scale: float32 [2, 48, 1024], P(None, 'rep', 'tp')
- o_served: bfloat16 [2, 6144, 6144], P(None, 'tp', 'rep')
- o_scale: float32 [2, 48, 6144], P(None, 'tp', 'rep')
- gate_served: bfloat16 [2, 6144, 16384], P(None, 'rep', 'tp')
- gate_scale: float32 [2, 48, 16384], P(None, 'rep', 'tp')
- up_served: bfloat16 [2, 6144, 16384], P(None, 'rep', 'tp')
- up_scale: float32 [2, 48, 16384], P(None, 'rep', 'tp')
The draws below stay inside these ranges and needn't reach their ends.
All inputs are finite; a program needn't handle non-finite values. Where the reference program divides by a largest or mean magnitude, that divisor is 1e-20 or more.
Results may differ from the reference program's by a relative error of at most 0.001.
Values may be sent and summed in bfloat16 or wider, within the bound.
A program may use at most 192 MiB of HBM per device.

```python
import math
import jax
import jax.numpy as jnp
from jax import lax

D = 6144
KV = 1024
FF = 16384
GROUP = 128
LAYERS = 2
PADMAX = 2
FLAT_DEV = 18091008
FLAT = 578912256
DEVICES = 32


def draw_flat_buffer(key, part):
    first, second = jax.random.split(jax.random.fold_in(key, 17))
    base = jnp.clip(jax.random.normal(first, (FLAT,), jnp.float32), -6.0, 6.0)
    factor = jnp.exp(jax.random.uniform(second, (FLAT // 32,), jnp.float32, 0.0, math.log(10.0)))
    return (base * jnp.repeat(factor, 32)).astype(jnp.bfloat16)


def touch_ends(result, rng, low, high):
    longest = result.shape.index(max(result.shape))
    spots = []
    for shift in (0, 1):
        where = [jax.random.randint(jax.random.fold_in(rng, axis), (), 0, length) for axis, length in enumerate(result.shape)]
        where[longest] = (where[longest] + shift) % result.shape[longest]
        spots.append(tuple(where))
    return result.at[spots[0]].set(low).at[spots[1]].set(high)


def setup_inputs(seed: int = 0) -> dict:
    streams_of = jax.random.split(jax.random.key(seed), 3)
    flat_buffer = draw_flat_buffer(jax.random.fold_in(streams_of[2], 71), 0)
    shard_pad = touch_ends(jax.random.randint(streams_of[1], (LAYERS, 6), 0, PADMAX + 1), jax.random.fold_in(streams_of[1], 1), 0, PADMAX).astype(jnp.int32)
    return {"flat_buffer": flat_buffer, "shard_pad": shard_pad}


def quantize(served):
    values = served.astype(jnp.float32)
    grouped = values.reshape(values.shape[0] // GROUP, GROUP, values.shape[1])
    peak = jnp.max(jnp.abs(grouped), axis=1) + 1e-6
    scaled = (grouped / peak[:, None, :]).astype(jnp.bfloat16)
    return scaled.reshape(served.shape), peak


def reference(flat_buffer, shard_pad):
    widths = (D, KV, KV, D, FF, FF)
    table = flat_buffer.reshape(DEVICES, FLAT_DEV)
    offset = jnp.zeros((), jnp.int32)
    served_all = [[] for index in range(6)]
    scale_all = [[] for index in range(6)]
    for layer in range(LAYERS):
        for index in range(6):
            length = widths[index] // DEVICES * D
            piece = lax.dynamic_slice_in_dim(table, offset.astype(jnp.int32), length, 1)
            whole = piece.reshape(widths[index], D)
            scaled, peak = quantize(whole.T)
            served_all[index].append(scaled)
            scale_all[index].append(peak)
            offset = (offset + length + 128 * shard_pad[layer, index]).astype(jnp.int32)
    outputs = []
    for index in range(6):
        outputs.append(jnp.stack(served_all[index]))
        outputs.append(jnp.stack(scale_all[index]))
    return (outputs[0], outputs[1], outputs[2], outputs[3], outputs[4], outputs[5],
            outputs[6], outputs[7], outputs[8], outputs[9], outputs[10], outputs[11])
```

```python
import functools
import math

import jax
import jax.numpy as jnp
import numpy as np
from jax import lax
from jax.experimental import pallas as pl
from jax.experimental.pallas import tpu as pltpu
from jax.sharding import PartitionSpec as P

D = 6144
KV = 1024
FF = 16384
GROUP = 128
LAYERS = 2
WIDTHS = (D, KV, KV, D, FF, FF)
LINES = D // GROUP
ORDER = [(index, layer) for index in (0, 1, 2, 4, 5) for layer in range(LAYERS)]
CHUNKS = 16
AHEAD = 2


def prepare_kernel(starts, window, out, wide):
    rows = out.shape[1]
    shift = starts[pl.program_id(0)] % 8
    wide[...] = window[...].astype(jnp.float32)
    for line in range(LINES):
        picked = wide[pl.ds(shift + line, rows, stride=LINES), :]
        out[line] = picked.astype(jnp.bfloat16)


def prepare(tiled, starts, rows):
    steps = starts.shape[0]
    span = rows * LINES + 8
    return pl.pallas_call(
        prepare_kernel,
        grid_spec=pltpu.PrefetchScalarGridSpec(
            num_scalar_prefetch=1,
            grid=(steps,),
            in_specs=[
                pl.BlockSpec(
                    (pl.Element(span), pl.Element(GROUP)),
                    lambda i, starts: (pl.multiple_of(starts[i] // 8 * 8, 8), 0),
                )
            ],
            out_specs=pl.BlockSpec((LINES, rows, GROUP), lambda i, starts: (0, i, 0)),
            scratch_shapes=[pltpu.VMEM((span, GROUP), jnp.float32)],
        ),
        out_shape=jax.ShapeDtypeStruct((LINES, steps * rows, GROUP), jnp.bfloat16),
        cost_estimate=pl.CostEstimate(
            flops=4 * steps * span * GROUP,
            bytes_accessed=4 * steps * span * GROUP,
            transcendentals=0,
        ),
    )(starts, tiled)


def exchange_kernel(reps, tps, sent, arrived, passing, send_a, recv_a, send_b, recv_b, kept):
    rep = lax.axis_index("rep")
    tp = lax.axis_index("tp")
    ratio = reps // tps
    depth = LINES // reps
    rows = sent.shape[1] // CHUNKS
    target = rep // ratio

    def at(device_rep, device_tp):
        return dict(
            device_id=(device_rep, device_tp), device_id_type=pl.DeviceIdType.MESH
        )

    barrier = pltpu.get_barrier_semaphore()
    for hop in range(1, reps):
        pl.semaphore_signal(barrier, inc=1, **at((rep + hop) % reps, tp))
    for hop in range(1, tps):
        pl.semaphore_signal(barrier, inc=1, **at(rep, (tp + hop) % tps))
    pl.semaphore_wait(barrier, reps + tps - 2)

    def block(chunk):
        return pl.ds(pl.multiple_of(chunk * rows, 8), rows)

    def mine(chunk, owner):
        return sent.at[pl.ds(owner * depth, depth), block(chunk)]

    def spread(chunk):
        for hop in range(1, reps):
            owner = (rep + hop) % reps

            def go(place):
                pltpu.make_async_remote_copy(
                    src_ref=mine(chunk, owner),
                    dst_ref=place,
                    send_sem=send_a.at[chunk],
                    recv_sem=recv_a.at[chunk],
                    **at(owner, tp),
                ).start()

            @pl.when(target == tp)
            def _():
                go(arrived.at[tp, rep % ratio, :, block(chunk)])

            @pl.when(target != tp)
            def _():
                go(passing.at[rep, :, block(chunk)])

    def forward(chunk):
        for hop in range(1, tps):
            there = (tp + hop) % tps
            for part in range(ratio):
                source = there * ratio + part

                def go(data):
                    pltpu.make_async_remote_copy(
                        src_ref=data,
                        dst_ref=arrived.at[tp, part, :, block(chunk)],
                        send_sem=send_b.at[chunk],
                        recv_sem=recv_b.at[chunk],
                        **at(rep, there),
                    ).start()

                @pl.when(source == rep)
                def _():
                    go(mine(chunk, rep))

                @pl.when(source != rep)
                def _():
                    go(passing.at[source, :, block(chunk)])

    @pl.when(target == tp)
    def _():
        pltpu.make_async_copy(
            sent.at[pl.ds(rep * depth, depth)], arrived.at[tp, rep % ratio], kept
        ).start()

    for chunk in range(AHEAD):
        spread(chunk)

    def wait(semaphore, chunk, count):
        whole = passing.at[pl.ds(0, count), :, block(chunk)]
        pltpu.make_async_copy(whole, whole, semaphore.at[chunk]).wait()

    @pl.loop(0, CHUNKS)
    def _(chunk):
        @pl.when(chunk + AHEAD < CHUNKS)
        def _():
            spread(chunk + AHEAD)

        wait(recv_a, chunk, reps - 1)
        forward(chunk)

    @pl.loop(0, CHUNKS)
    def _(chunk):
        wait(send_a, chunk, reps - 1)
        wait(send_b, chunk, ratio * (tps - 1))
        wait(recv_b, chunk, ratio * (tps - 1))

    @pl.when(target == tp)
    def _():
        pltpu.make_async_copy(
            sent.at[pl.ds(rep * depth, depth)], arrived.at[tp, rep % ratio], kept
        ).wait()


def exchange(sent, reps, tps):
    rows = sent.shape[1]
    depth = LINES // reps
    size = 2 * sent.size
    arrived, _ = pl.pallas_call(
        functools.partial(exchange_kernel, reps, tps),
        in_specs=[pl.BlockSpec(memory_space=pl.ANY)],
        out_specs=[pl.BlockSpec(memory_space=pl.ANY)] * 2,
        out_shape=[
            jax.ShapeDtypeStruct((tps, reps // tps, depth, rows, GROUP), jnp.bfloat16),
            jax.ShapeDtypeStruct((reps, depth, rows, GROUP), jnp.bfloat16),
        ],
        scratch_shapes=[pltpu.SemaphoreType.DMA((CHUNKS,))] * 4
        + [pltpu.SemaphoreType.DMA],
        compiler_params=pltpu.CompilerParams(collective_id=0, has_side_effects=True),
        cost_estimate=pl.CostEstimate(
            flops=0, bytes_accessed=60 * size, transcendentals=0
        ),
    )(sent)
    return arrived


def quantize_kernel(order, *refs):
    received, (scaled, scale) = refs[:-2], refs[-2:]
    group = pl.program_id(1)

    def run(ref):
        parts = [ref[where + (0,)] for where in order]
        served = jnp.concatenate(parts, axis=0).T.astype(jnp.float32)
        peak = jnp.max(jnp.abs(served), axis=0, keepdims=True) + 1e-06
        scaled[0] = (served * (1.0 / peak)).astype(jnp.bfloat16)
        scale[0, pl.ds(group, 1), :] = peak

    if len(received) == 1:
        run(received[0])
    else:
        for layer, ref in enumerate(received):
            pl.when(pl.program_id(0) == layer)(functools.partial(run, ref))


def quantize(received, order, groups, rows, places, earlier=()):
    total = len(order) * rows
    lead = received.shape[:-3]
    zeros = (0,) * len(lead)
    first, base = places[0]
    layers = len(places)
    return pl.pallas_call(
        lambda *refs: quantize_kernel(order, refs[0], refs[-2], refs[-1]),
        grid=(layers, groups),
        in_specs=[
            pl.BlockSpec(
                lead + (1, rows, GROUP), lambda l, g: zeros + (g, base + l, 0)
            )
        ]
        + [pl.BlockSpec(memory_space=pl.ANY)] * len(earlier),
        out_specs=[
            pl.BlockSpec((1, GROUP, total), lambda l, g: (first + l, g, 0)),
            pl.BlockSpec((1, groups, total), lambda l, g: (first + l, 0, 0)),
        ],
        out_shape=[
            jax.ShapeDtypeStruct((LAYERS, groups * GROUP, total), jnp.bfloat16),
            jax.ShapeDtypeStruct((LAYERS, groups, total), jnp.float32),
        ],
        input_output_aliases={1 + i: i for i in range(len(earlier))},
        cost_estimate=pl.CostEstimate(
            flops=20 * layers * groups * GROUP * total,
            bytes_accessed=4 * layers * groups * GROUP * total,
            transcendentals=0,
        ),
    )(received, *earlier)


def on_device(flat_buffer, shard_pad):
    reps = lax.axis_size("rep")
    tps = lax.axis_size("tp")
    devices = reps * tps
    ratio = reps // tps
    rows = [width // devices for width in WIDTHS]
    tiled = flat_buffer.reshape(flat_buffer.shape[0] // GROUP, GROUP)
    bases = np.concatenate([[0], np.cumsum(rows * LAYERS)[:-1]]) * LINES
    pads = shard_pad.reshape(-1)

    def starts(tensors, step):
        base, before = [], []
        for index, layer in tensors:
            place = layer * len(WIDTHS) + index
            for row in range(0, rows[index], step):
                base.append(bases[place] + row * LINES)
                before.append(np.arange(pads.shape[0]) < place)
        before = jnp.asarray(np.array(before))
        shifts = jnp.sum(jnp.where(before, pads[None, :], 0), axis=1)
        return shifts + jnp.asarray(np.array(base, np.int32))

    wide = math.gcd(rows[3], 96)
    step = math.gcd(*rows)
    sent_o = [prepare(tiled, starts([(3, layer)], wide), wide) for layer in range(LAYERS)]
    sent = prepare(tiled, starts(ORDER, step), step)

    def across(piece):
        got = lax.all_to_all(piece, "tp", split_axis=0, concat_axis=0, tiled=True)
        return got.reshape(tps, LINES // tps, rows[3], GROUP)

    early = across(sent_o[0])
    arrived = exchange(sent, reps, tps)
    arrived, late = lax.optimization_barrier((arrived, sent_o[1]))
    late = across(late)

    outputs = [()] * len(WIDTHS)
    order = [(where, part) for part in range(ratio) for where in range(tps)]
    begin = 0
    for index in (0, 1, 2, 4, 5):
        outputs[index] = quantize(
            arrived, order, LINES // reps, rows[index], [(0, begin // rows[index]), (1, 0)]
        )
        begin += LAYERS * rows[index]
    order = [(where,) for where in range(tps)]
    part = quantize(early, order, LINES // tps, rows[3], [(0, 0)])
    outputs[3] = quantize(late, order, LINES // tps, rows[3], [(1, 0)], tuple(part))
    return tuple(array for pair in outputs for array in pair)


def solution(mesh):
    column = P(None, "rep", "tp")
    row = P(None, "tp", "rep")
    return jax.shard_map(
        on_device,
        mesh=mesh,
        in_specs=(P(("rep", "tp")), P()),
        out_specs=(column,) * 6 + (row,) * 2 + (column,) * 4,
        check_vma=False,
    )
```

```python
import functools
import math

import jax
import jax.numpy as jnp
import numpy as np
from jax import lax
from jax.experimental import pallas as pl
from jax.experimental.pallas import tpu as pltpu
from jax.sharding import PartitionSpec as P

D = 6144
KV = 1024
FF = 16384
GROUP = 128
LAYERS = 2
WIDTHS = (D, KV, KV, D, FF, FF)
LINES = D // GROUP
ORDER = [(index, layer) for index in (0, 1, 2, 4, 5) for layer in range(LAYERS)]
CHUNKS = 16
PITCH = LINES + 4
AHEAD = 2


def prepare_kernel(pieces, starts, *refs):
    windows, out, wide = refs[:pieces], refs[pieces], refs[pieces + 1]
    rows = out.shape[1] // pieces
    pitch = wide.shape[0] // (rows + 1)
    for piece, window in enumerate(windows):
        shift = starts[pl.program_id(0) * pieces + piece] % 8
        for row in range(rows + 1):
            count = min(LINES, window.shape[0] - row * LINES)
            wide[pl.ds(row * pitch, count), :] = window[
                pl.ds(row * LINES, count), :
            ].astype(jnp.float32)
        for line in range(LINES):
            first = shift + line
            first = jnp.where(first < LINES, first, first + pitch - LINES)
            picked = wide[pl.ds(first, rows, stride=pitch), :]
            out[line, pl.ds(piece * rows, rows)] = picked.astype(jnp.bfloat16)


def prepare(tiled, starts, rows, pieces):
    steps = starts.shape[0] // pieces
    span = rows * LINES + 8

    def window(piece):
        return pl.BlockSpec(
            (pl.Element(span), pl.Element(GROUP)),
            lambda i, starts: (
                pl.multiple_of(starts[i * pieces + piece] // 8 * 8, 8),
                0,
            ),
        )

    return pl.pallas_call(
        functools.partial(prepare_kernel, pieces),
        grid_spec=pltpu.PrefetchScalarGridSpec(
            num_scalar_prefetch=1,
            grid=(steps,),
            in_specs=[window(piece) for piece in range(pieces)],
            out_specs=pl.BlockSpec(
                (LINES, pieces * rows, GROUP), lambda i, starts: (0, i, 0)
            ),
            scratch_shapes=[pltpu.VMEM(((rows + 1) * PITCH, GROUP), jnp.float32)],
        ),
        out_shape=jax.ShapeDtypeStruct(
            (LINES, steps * pieces * rows, GROUP), jnp.bfloat16
        ),
        cost_estimate=pl.CostEstimate(
            flops=4 * steps * pieces * span * GROUP,
            bytes_accessed=4 * steps * pieces * span * GROUP,
            transcendentals=0,
        ),
    )(starts, *[tiled] * pieces)


def exchange_kernel(reps, tps, sent, arrived, passing, send_a, recv_a, send_b, recv_b, kept):
    rep = lax.axis_index("rep")
    tp = lax.axis_index("tp")
    ratio = reps // tps
    depth = LINES // reps
    rows = sent.shape[1] // CHUNKS
    target = rep // ratio

    def at(device_rep, device_tp):
        return dict(
            device_id=(device_rep, device_tp), device_id_type=pl.DeviceIdType.MESH
        )

    barrier = pltpu.get_barrier_semaphore()
    for hop in range(1, reps):
        pl.semaphore_signal(barrier, inc=1, **at((rep + hop) % reps, tp))
    for hop in range(1, tps):
        pl.semaphore_signal(barrier, inc=1, **at(rep, (tp + hop) % tps))
    pl.semaphore_wait(barrier, reps + tps - 2)

    def block(chunk):
        return pl.ds(pl.multiple_of(chunk * rows, 8), rows)

    def mine(chunk, owner):
        return sent.at[pl.ds(owner * depth, depth), block(chunk)]

    def spread(chunk):
        for hop in range(1, reps):
            owner = (rep + hop) % reps

            def go(place):
                pltpu.make_async_remote_copy(
                    src_ref=mine(chunk, owner),
                    dst_ref=place,
                    send_sem=send_a.at[chunk],
                    recv_sem=recv_a.at[chunk],
                    **at(owner, tp),
                ).start()

            @pl.when(target == tp)
            def _():
                go(arrived.at[tp, rep % ratio, :, block(chunk)])

            @pl.when(target != tp)
            def _():
                go(passing.at[rep, :, block(chunk)])

    def forward(chunk):
        for hop in range(1, tps):
            there = (tp + hop) % tps
            for part in range(ratio):
                source = there * ratio + part

                def go(data):
                    pltpu.make_async_remote_copy(
                        src_ref=data,
                        dst_ref=arrived.at[tp, part, :, block(chunk)],
                        send_sem=send_b.at[chunk],
                        recv_sem=recv_b.at[chunk],
                        **at(rep, there),
                    ).start()

                @pl.when(source == rep)
                def _():
                    go(mine(chunk, rep))

                @pl.when(source != rep)
                def _():
                    go(passing.at[source, :, block(chunk)])

    @pl.when(target == tp)
    def _():
        pltpu.make_async_copy(
            sent.at[pl.ds(rep * depth, depth)], arrived.at[tp, rep % ratio], kept
        ).start()

    for chunk in range(AHEAD):
        spread(chunk)

    def wait(semaphore, chunk, count):
        whole = passing.at[pl.ds(0, count), :, block(chunk)]
        pltpu.make_async_copy(whole, whole, semaphore.at[chunk]).wait()

    @pl.loop(0, CHUNKS)
    def _(chunk):
        @pl.when(chunk + AHEAD < CHUNKS)
        def _():
            spread(chunk + AHEAD)

        wait(recv_a, chunk, reps - 1)
        forward(chunk)

    @pl.loop(0, CHUNKS)
    def _(chunk):
        wait(send_a, chunk, reps - 1)
        wait(send_b, chunk, ratio * (tps - 1))
        wait(recv_b, chunk, ratio * (tps - 1))

    @pl.when(target == tp)
    def _():
        pltpu.make_async_copy(
            sent.at[pl.ds(rep * depth, depth)], arrived.at[tp, rep % ratio], kept
        ).wait()


def exchange(sent, reps, tps):
    rows = sent.shape[1]
    depth = LINES // reps
    size = 2 * sent.size
    arrived, _ = pl.pallas_call(
        functools.partial(exchange_kernel, reps, tps),
        in_specs=[pl.BlockSpec(memory_space=pl.ANY)],
        out_specs=[pl.BlockSpec(memory_space=pl.ANY)] * 2,
        out_shape=[
            jax.ShapeDtypeStruct((tps, reps // tps, depth, rows, GROUP), jnp.bfloat16),
            jax.ShapeDtypeStruct((reps, depth, rows, GROUP), jnp.bfloat16),
        ],
        scratch_shapes=[pltpu.SemaphoreType.DMA((CHUNKS,))] * 4
        + [pltpu.SemaphoreType.DMA],
        compiler_params=pltpu.CompilerParams(collective_id=0, has_side_effects=True),
        cost_estimate=pl.CostEstimate(
            flops=0, bytes_accessed=60 * size, transcendentals=0
        ),
    )(sent)
    return arrived


def columns(order, rows):
    width = math.gcd(rows, 256)
    chunks, chunk, size = [], [], 0
    for where in order:
        for begin in range(0, rows, width):
            chunk.append((where, begin, width))
            size += width
            if size % GROUP == 0 and size >= 256:
                chunks.append(chunk)
                chunk, size = [], 0
    return chunks + [chunk] if chunk else chunks


def quantize_kernel(chunks, members, first, *refs):
    tensors = len(members)
    received = refs[: sum(members)]
    outputs = refs[-2 * tensors :]
    taken = 0
    for tensor in range(tensors):
        scaled, scale = outputs[2 * tensor], outputs[2 * tensor + 1]
        if first:
            for before in range(first):
                scale[:, before] = refs[-2 * tensors - 1][:, before]
        for member in range(members[tensor]):
            data = received[taken]
            taken += 1
            for group in range(scale.shape[0]):
                column = 0
                for chunk in chunks:
                    parts = [
                        data[where + (group, pl.ds(begin, width))]
                        for where, begin, width in chunk
                    ]
                    part = parts[0] if len(parts) == 1 else jnp.concatenate(parts, axis=0)
                    served = part.T.astype(jnp.float32)
                    peak = jnp.max(jnp.abs(served), axis=0, keepdims=True) + 1e-06
                    across = pl.ds(column, part.shape[0])
                    scaled[member, pl.ds(group * GROUP, GROUP), across] = (
                        served * (1.0 / peak)
                    ).astype(jnp.bfloat16)
                    scale[group, pl.ds(first + member, 1), across] = peak
                    column += part.shape[0]


def quantize(received, order, groups, rows, places, batch, first=0, earlier=()):
    total = len(order) * rows
    lead = received.shape[:-3]
    zeros = (0,) * len(lead)
    members = [len(place) for place in places]
    layers = members[0]
    flat = [base for place in places for base in place]

    def source(base):
        return pl.BlockSpec(
            lead + (batch, rows, GROUP), lambda g: zeros + (g, base, 0)
        )

    scale = pl.BlockSpec((batch, LAYERS, total), lambda g: (g, 0, 0))
    outputs = pl.pallas_call(
        functools.partial(quantize_kernel, columns(order, rows), members, first),
        grid=(groups // batch,),
        in_specs=[source(base) for base in flat]
        + [pl.BlockSpec(memory_space=pl.ANY), scale][: len(earlier)],
        out_specs=[
            pl.BlockSpec(
                (layers, batch * GROUP, total), lambda g: (first // layers, g, 0)
            ),
            scale,
        ]
        * len(places),
        out_shape=[
            jax.ShapeDtypeStruct((LAYERS, groups * GROUP, total), jnp.bfloat16),
            jax.ShapeDtypeStruct((groups, LAYERS, total), jnp.float32),
        ]
        * len(places),
        input_output_aliases={len(flat): 0} if earlier else {},
        cost_estimate=pl.CostEstimate(
            flops=20 * len(flat) * groups * GROUP * total,
            bytes_accessed=4 * len(flat) * groups * GROUP * total,
            transcendentals=0,
        ),
    )(*[received] * len(flat), *earlier)
    return [tuple(outputs[2 * i : 2 * i + 2]) for i in range(len(places))]


def on_device(flat_buffer, shard_pad):
    reps = lax.axis_size("rep")
    tps = lax.axis_size("tp")
    devices = reps * tps
    ratio = reps // tps
    rows = [width // devices for width in WIDTHS]
    tiled = flat_buffer.reshape(flat_buffer.shape[0] // GROUP, GROUP)
    bases = np.concatenate([[0], np.cumsum(rows * LAYERS)[:-1]]) * LINES
    pads = shard_pad.reshape(-1)

    def starts(tensors, step):
        base, before = [], []
        for index, layer in tensors:
            place = layer * len(WIDTHS) + index
            for row in range(0, rows[index], step):
                base.append(bases[place] + row * LINES)
                before.append(np.arange(pads.shape[0]) < place)
        before = jnp.asarray(np.array(before))
        shifts = jnp.sum(jnp.where(before, pads[None, :], 0), axis=1)
        return shifts + jnp.asarray(np.array(base, np.int32))

    wide = math.gcd(rows[3], 96)
    sent_o = [
        prepare(tiled, starts([(3, layer)], wide), wide, 1) for layer in range(LAYERS)
    ]
    step = math.gcd(*rows)
    sent = prepare(tiled, starts(ORDER, step), step, math.gcd(rows[4] // step, 4))

    def across(piece):
        got = lax.all_to_all(piece, "tp", split_axis=0, concat_axis=0, tiled=True)
        return got.reshape(tps, LINES // tps, rows[3], GROUP)

    early = across(sent_o[0])
    arrived = exchange(sent, reps, tps)
    arrived, late = lax.optimization_barrier((arrived, sent_o[1]))
    late = across(late)

    begin, bases = 0, {}
    for index, layer in ORDER:
        bases[index, layer] = begin // rows[index]
        begin += rows[index]
    places = {
        index: [bases[index, layer] for layer in range(LAYERS)]
        for index in (0, 1, 2, 4, 5)
    }
    order = [(where, part) for part in range(ratio) for where in range(tps)]
    depth = LINES // reps
    outputs = [None] * len(WIDTHS)
    for batch, tensors in ((2, (4,)), (2, (5,)), (depth, (0,)), (depth, (1, 2))):
        done = quantize(
            arrived,
            order,
            depth,
            rows[tensors[0]],
            [places[index] for index in tensors],
            math.gcd(batch, depth),
        )
        for index, pair in zip(tensors, done):
            outputs[index] = pair
    order = [(where,) for where in range(tps)]
    depth = LINES // tps
    batch = math.gcd(depth, 4)
    part = quantize(early, order, depth, rows[3], [[0]], batch)[0]
    outputs[3] = quantize(late, order, depth, rows[3], [[0]], batch, 1, part)[0]
    return tuple(
        array for scaled, scale in outputs for array in (scaled, scale.transpose(1, 0, 2))
    )


def solution(mesh):
    column = P(None, "rep", "tp")
    row = P(None, "tp", "rep")
    return jax.shard_map(
        on_device,
        mesh=mesh,
        in_specs=(P(("rep", "tp")), P()),
        out_specs=(column,) * 6 + (row,) * 2 + (column,) * 4,
        check_vma=False,
    )
```

```python
import functools
import math

import jax
import jax.numpy as jnp
import numpy as np
from jax import lax
from jax.experimental import pallas as pl
from jax.experimental.pallas import tpu as pltpu
from jax.sharding import PartitionSpec as P

D = 6144
KV = 1024
FF = 16384
GROUP = 128
LAYERS = 2
WIDTHS = (D, KV, KV, D, FF, FF)
LINES = D // GROUP
ORDER = [(index, layer) for index in (0, 1, 2, 4, 5) for layer in range(LAYERS)]
CHUNKS = 32
PITCH = LINES + 4
AHEAD = 4


def prepare_kernel(pieces, starts, *refs):
    windows, out, wide = refs[:pieces], refs[pieces], refs[pieces + 1]
    rows = out.shape[1] // pieces
    pitch = wide.shape[0] // (rows + 1)
    for piece, window in enumerate(windows):
        shift = starts[pl.program_id(0) * pieces + piece] % 8
        for row in range(rows + 1):
            count = min(LINES, window.shape[0] - row * LINES)
            wide[pl.ds(row * pitch, count), :] = window[
                pl.ds(row * LINES, count), :
            ].astype(jnp.float32)
        for line in range(LINES):
            first = shift + line
            first = jnp.where(first < LINES, first, first + pitch - LINES)
            picked = wide[pl.ds(first, rows, stride=pitch), :]
            out[line, pl.ds(piece * rows, rows)] = picked.astype(jnp.bfloat16)


def prepare(tiled, starts, rows, pieces):
    steps = starts.shape[0] // pieces
    span = rows * LINES + 8

    def window(piece):
        return pl.BlockSpec(
            (pl.Element(span), pl.Element(GROUP)),
            lambda i, starts: (
                pl.multiple_of(starts[i * pieces + piece] // 8 * 8, 8),
                0,
            ),
        )

    return pl.pallas_call(
        functools.partial(prepare_kernel, pieces),
        grid_spec=pltpu.PrefetchScalarGridSpec(
            num_scalar_prefetch=1,
            grid=(steps,),
            in_specs=[window(piece) for piece in range(pieces)],
            out_specs=pl.BlockSpec(
                (LINES, pieces * rows, GROUP), lambda i, starts: (0, i, 0)
            ),
            scratch_shapes=[pltpu.VMEM(((rows + 1) * PITCH, GROUP), jnp.float32)],
        ),
        out_shape=jax.ShapeDtypeStruct(
            (LINES, steps * pieces * rows, GROUP), jnp.bfloat16
        ),
        cost_estimate=pl.CostEstimate(
            flops=4 * steps * pieces * span * GROUP,
            bytes_accessed=4 * steps * pieces * span * GROUP,
            transcendentals=0,
        ),
    )(starts, *[tiled] * pieces)


def rotate_kernel(base, place, tps, pads, window, *refs):
    outs, wide = refs[:-1], refs[-1]
    depth, rows = outs[0].shape[:2]
    pitch = wide.shape[0] // (rows + 1)
    tp = lax.axis_index("tp")
    shift = begin(base, place, pads) % 8
    for row in range(rows + 1):
        count = min(LINES, window.shape[0] - row * LINES)
        wide[pl.ds(row * pitch, count), :] = window[pl.ds(row * LINES, count), :].astype(
            jnp.float32
        )
    for hop, out in enumerate(outs):
        for line in range(depth):
            first = shift + (tp + hop) % tps * depth + line
            first = jnp.where(first < LINES, first, first + pitch - LINES)
            picked = wide[pl.ds(first, rows, stride=pitch), :]
            out[line] = picked.astype(jnp.bfloat16)


def begin(base, place, pads):
    start = base
    for earlier in range(place):
        start = start + pads[earlier // len(WIDTHS), earlier % len(WIDTHS)]
    return start


def rotate(tiled, pads, base, place, rows, step, tps):
    depth = LINES // tps
    span = step * LINES + 8

    def window(i, pads):
        start = begin(base, place, pads) + i * step * LINES
        return (pl.multiple_of(start // 8 * 8, 8), 0)

    return pl.pallas_call(
        functools.partial(rotate_kernel, base, place, tps),
        grid_spec=pltpu.PrefetchScalarGridSpec(
            num_scalar_prefetch=1,
            grid=(rows // step,),
            in_specs=[pl.BlockSpec((pl.Element(span), pl.Element(GROUP)), window)],
            out_specs=[
                pl.BlockSpec((depth, step, GROUP), lambda i, pads: (0, i, 0))
            ]
            * tps,
            scratch_shapes=[pltpu.VMEM(((step + 1) * PITCH, GROUP), jnp.float32)],
        ),
        out_shape=[jax.ShapeDtypeStruct((depth, rows, GROUP), jnp.bfloat16)] * tps,
        cost_estimate=pl.CostEstimate(
            flops=4 * rows * D, bytes_accessed=4 * rows * D, transcendentals=0
        ),
    )(pads, tiled)


def exchange_kernel(reps, tps, sent, arrived, passing, send_a, recv_a, send_b, recv_b, kept):
    rep = lax.axis_index("rep")
    tp = lax.axis_index("tp")
    ratio = reps // tps
    depth = LINES // reps
    chunks = math.gcd(sent.shape[1] // 8, CHUNKS)
    rows = sent.shape[1] // chunks
    target = rep // ratio

    def at(device_rep, device_tp):
        return dict(
            device_id=(device_rep, device_tp), device_id_type=pl.DeviceIdType.MESH
        )

    barrier = pltpu.get_barrier_semaphore()
    for hop in range(1, reps):
        pl.semaphore_signal(barrier, inc=1, **at((rep + hop) % reps, tp))
    for hop in range(1, tps):
        pl.semaphore_signal(barrier, inc=1, **at(rep, (tp + hop) % tps))
    pl.semaphore_wait(barrier, reps + tps - 2)

    def block(chunk):
        return pl.ds(pl.multiple_of(chunk * rows, 8), rows)

    def mine(chunk, owner):
        return sent.at[pl.ds(owner * depth, depth), block(chunk)]

    def spread(chunk):
        for hop in range(1, reps):
            owner = (rep + hop) % reps

            def go(place):
                pltpu.make_async_remote_copy(
                    src_ref=mine(chunk, owner),
                    dst_ref=place,
                    send_sem=send_a.at[chunk],
                    recv_sem=recv_a.at[chunk],
                    **at(owner, tp),
                ).start()

            @pl.when(target == tp)
            def _():
                go(arrived.at[tp, rep % ratio, :, block(chunk)])

            @pl.when(target != tp)
            def _():
                go(passing.at[rep, :, block(chunk)])

    def forward(chunk):
        for hop in range(1, tps):
            there = (tp + hop) % tps
            for part in range(ratio):
                source = there * ratio + part

                def go(data):
                    pltpu.make_async_remote_copy(
                        src_ref=data,
                        dst_ref=arrived.at[tp, part, :, block(chunk)],
                        send_sem=send_b.at[chunk],
                        recv_sem=recv_b.at[chunk],
                        **at(rep, there),
                    ).start()

                @pl.when(source == rep)
                def _():
                    go(mine(chunk, rep))

                @pl.when(source != rep)
                def _():
                    go(passing.at[source, :, block(chunk)])

    @pl.when(target == tp)
    def _():
        pltpu.make_async_copy(
            sent.at[pl.ds(rep * depth, depth)], arrived.at[tp, rep % ratio], kept
        ).start()

    for chunk in range(AHEAD):
        spread(chunk)

    def wait(semaphore, chunk, count):
        whole = passing.at[pl.ds(0, count), :, block(chunk)]
        pltpu.make_async_copy(whole, whole, semaphore.at[chunk]).wait()

    @pl.loop(0, chunks)
    def _(chunk):
        @pl.when(chunk + AHEAD < chunks)
        def _():
            spread(chunk + AHEAD)

        wait(recv_a, chunk, reps - 1)
        forward(chunk)

    @pl.loop(0, chunks)
    def _(chunk):
        wait(send_a, chunk, reps - 1)
        wait(send_b, chunk, ratio * (tps - 1))
        wait(recv_b, chunk, ratio * (tps - 1))

    @pl.when(target == tp)
    def _():
        pltpu.make_async_copy(
            sent.at[pl.ds(rep * depth, depth)], arrived.at[tp, rep % ratio], kept
        ).wait()


def exchange(sent, reps, tps):
    rows = sent.shape[1]
    depth = LINES // reps
    size = 2 * sent.size
    arrived, _ = pl.pallas_call(
        functools.partial(exchange_kernel, reps, tps),
        in_specs=[pl.BlockSpec(memory_space=pl.ANY)],
        out_specs=[pl.BlockSpec(memory_space=pl.ANY)] * 2,
        out_shape=[
            jax.ShapeDtypeStruct((tps, reps // tps, depth, rows, GROUP), jnp.bfloat16),
            jax.ShapeDtypeStruct((reps, depth, rows, GROUP), jnp.bfloat16),
        ],
        scratch_shapes=[pltpu.SemaphoreType.DMA((CHUNKS,))] * 4
        + [pltpu.SemaphoreType.DMA],
        compiler_params=pltpu.CompilerParams(collective_id=0, has_side_effects=True),
        cost_estimate=pl.CostEstimate(
            flops=0, bytes_accessed=60 * size, transcendentals=0
        ),
    )(sent)
    return arrived


def columns(order, rows):
    width = math.gcd(rows, 256)
    chunks, chunk, size = [], [], 0
    for where in order:
        for begin in range(0, rows, width):
            chunk.append((where, begin, width))
            size += width
            if size % GROUP == 0 and size >= 256:
                chunks.append(chunk)
                chunk, size = [], 0
    return chunks + [chunk] if chunk else chunks


def settle(parts, scaled, scale, member, layer, group, column):
    part = parts[0] if len(parts) == 1 else jnp.concatenate(parts, axis=0)
    served = part.T.astype(jnp.float32)
    peak = jnp.max(jnp.abs(served), axis=0, keepdims=True) + 1e-06
    across = pl.ds(column, part.shape[0])
    scaled[member, pl.ds(group * GROUP, GROUP), across] = (
        served * (1.0 / peak)
    ).astype(jnp.bfloat16)
    scale[group, pl.ds(layer, 1), across] = peak
    return column + part.shape[0]


def quantize_kernel(chunks, *refs):
    received, outputs = refs[: len(refs) // 2], refs[len(refs) // 2 :]
    for which, data in enumerate(received):
        tensor, layer = divmod(which, LAYERS)
        scaled, scale = outputs[2 * tensor], outputs[2 * tensor + 1]
        for group in range(scale.shape[0]):
            column = 0
            for chunk in chunks:
                parts = [
                    data[where + (group, pl.ds(begin, width))]
                    for where, begin, width in chunk
                ]
                column = settle(parts, scaled, scale, layer, layer, group, column)


def finish_kernel(chunks, tps, layer, *refs):
    received, scaled, scale = refs[:tps], refs[-2], refs[-1]
    for before in range(layer):
        scale[:, before] = refs[-3][:, before]

    def run(mine):
        for group in range(scale.shape[0]):
            column = 0
            for chunk in chunks:
                parts = [
                    received[(mine - where) % tps][group, pl.ds(begin, width)]
                    for where, begin, width in chunk
                ]
                column = settle(parts, scaled, scale, 0, layer, group, column)

    for mine in range(tps):
        pl.when(lax.axis_index("tp") == mine)(functools.partial(run, mine))


def finish(received, groups, rows, batch, layer, earlier=()):
    tps = len(received)
    total = tps * rows
    scale = pl.BlockSpec((batch, LAYERS, total), lambda g: (g, 0, 0))
    return pl.pallas_call(
        functools.partial(finish_kernel, columns(range(tps), rows), tps, layer),
        grid=(groups // batch,),
        in_specs=[pl.BlockSpec((batch, rows, GROUP), lambda g: (g, 0, 0))] * tps
        + [pl.BlockSpec(memory_space=pl.ANY), scale][: len(earlier)],
        out_specs=[
            pl.BlockSpec((1, batch * GROUP, total), lambda g: (layer, g, 0)),
            scale,
        ],
        out_shape=[
            jax.ShapeDtypeStruct((LAYERS, groups * GROUP, total), jnp.bfloat16),
            jax.ShapeDtypeStruct((groups, LAYERS, total), jnp.float32),
        ],
        input_output_aliases={tps: 0} if earlier else {},
        cost_estimate=pl.CostEstimate(
            flops=20 * groups * GROUP * total,
            bytes_accessed=4 * groups * GROUP * total,
            transcendentals=0,
        ),
    )(*received, *earlier)


def quantize(received, order, groups, rows, places, batch):
    total = len(order) * rows
    lead = received.shape[:-3]
    zeros = (0,) * len(lead)
    flat = [base for place in places for base in place]

    def source(base):
        return pl.BlockSpec(
            lead + (batch, rows, GROUP), lambda g: zeros + (g, base, 0)
        )

    outputs = pl.pallas_call(
        functools.partial(quantize_kernel, columns(order, rows)),
        grid=(groups // batch,),
        in_specs=[source(base) for base in flat],
        out_specs=[
            pl.BlockSpec((LAYERS, batch * GROUP, total), lambda g: (0, g, 0)),
            pl.BlockSpec((batch, LAYERS, total), lambda g: (g, 0, 0)),
        ]
        * len(places),
        out_shape=[
            jax.ShapeDtypeStruct((LAYERS, groups * GROUP, total), jnp.bfloat16),
            jax.ShapeDtypeStruct((groups, LAYERS, total), jnp.float32),
        ]
        * len(places),
        cost_estimate=pl.CostEstimate(
            flops=20 * len(flat) * groups * GROUP * total,
            bytes_accessed=4 * len(flat) * groups * GROUP * total,
            transcendentals=0,
        ),
    )(*[received] * len(flat))
    return [outputs[2 * i : 2 * i + 2] for i in range(len(places))]


def on_device(flat_buffer, shard_pad):
    reps = lax.axis_size("rep")
    tps = lax.axis_size("tp")
    devices = reps * tps
    ratio = reps // tps
    rows = [width // devices for width in WIDTHS]
    tiled = flat_buffer.reshape(flat_buffer.shape[0] // GROUP, GROUP)
    bases = np.concatenate([[0], np.cumsum(rows * LAYERS)[:-1]]) * LINES
    pads = shard_pad.reshape(-1)

    def starts(tensors, step):
        base, before = [], []
        for index, layer in tensors:
            place = layer * len(WIDTHS) + index
            for row in range(0, rows[index], step):
                base.append(bases[place] + row * LINES)
                before.append(np.arange(pads.shape[0]) < place)
        before = jnp.asarray(np.array(before))
        shifts = jnp.sum(jnp.where(before, pads[None, :], 0), axis=1)
        return shifts + jnp.asarray(np.array(base, np.int32))

    wide = math.gcd(rows[3], 96)
    sent_o = [
        rotate(tiled, shard_pad, int(bases[place]), place, rows[3], wide, tps)
        for place in (3, 3 + len(WIDTHS))
    ]

    def across(blocks):
        hops = sorted(range(1, tps), key=lambda hop: abs(2 * hop - tps))
        got = {
            hop: lax.ppermute(
                blocks[hop], "tp", [(at, (at + hop) % tps) for at in range(tps)]
            )
            for hop in hops
        }
        return [got.get(hop, blocks[0]) for hop in range(tps)]

    early = across(sent_o[0])
    step = math.gcd(*rows)
    sent = prepare(tiled, starts(ORDER, step), step, math.gcd(rows[4] // step, 4))
    sent, late = lax.optimization_barrier((sent, sent_o[1]))
    arrived = exchange(sent, reps, tps)
    arrived, late = lax.optimization_barrier((arrived, late))
    late = across(late)

    begins, bases = 0, {}
    for index, layer in ORDER:
        bases[index, layer] = begins // rows[index]
        begins += rows[index]
    places = {
        index: [bases[index, layer] for layer in range(LAYERS)]
        for index in (0, 1, 2, 4, 5)
    }
    order = [(where, part) for part in range(ratio) for where in range(tps)]
    depth = LINES // reps
    outputs = [None] * len(WIDTHS)
    for batch, tensors in ((2, (4,)), (2, (5,)), (depth, (0,)), (depth, (1, 2))):
        done = quantize(
            arrived,
            order,
            depth,
            rows[tensors[0]],
            [places[index] for index in tensors],
            math.gcd(batch, depth),
        )
        for index, pair in zip(tensors, done):
            outputs[index] = pair
    depth = LINES // tps
    batch = math.gcd(depth, 4)
    part = finish(early, depth, rows[3], batch, 0)
    outputs[3] = finish(late, depth, rows[3], batch, 1, tuple(part))
    return tuple(
        array for scaled, scale in outputs for array in (scaled, scale.transpose(1, 0, 2))
    )


def solution(mesh):
    column = P(None, "rep", "tp")
    row = P(None, "tp", "rep")
    return jax.shard_map(
        on_device,
        mesh=mesh,
        in_specs=(P(("rep", "tp")), P()),
        out_specs=(column,) * 6 + (row,) * 2 + (column,) * 4,
        check_vma=False,
    )
```

```python
import functools
import math

import jax
import jax.numpy as jnp
import numpy as np
from jax import lax
from jax.experimental import pallas as pl
from jax.experimental.pallas import tpu as pltpu
from jax.sharding import PartitionSpec as P

D = 6144
KV = 1024
FF = 16384
GROUP = 128
LAYERS = 2
WIDTHS = (D, KV, KV, D, FF, FF)
LINES = D // GROUP
ORDER = [(index, layer) for index in (0, 1, 2, 4, 5) for layer in range(LAYERS)]
CHUNKS = 32
PITCH = LINES + 4
AHEAD = 4
FIRST = 96


def prepare_kernel(pieces, starts, *refs):
    windows, out, wide = refs[:pieces], refs[pieces], refs[pieces + 1]
    rows = out.shape[1] // pieces
    pitch = wide.shape[0] // (rows + 1)
    for piece, window in enumerate(windows):
        shift = starts[pl.program_id(0) * pieces + piece] % 8
        for row in range(rows + 1):
            count = min(LINES, window.shape[0] - row * LINES)
            wide[pl.ds(row * pitch, count), :] = window[
                pl.ds(row * LINES, count), :
            ].astype(jnp.float32)
        for line in range(LINES):
            first = shift + line
            first = jnp.where(first < LINES, first, first + pitch - LINES)
            picked = wide[pl.ds(first, rows, stride=pitch), :]
            out[line, pl.ds(piece * rows, rows)] = picked.astype(jnp.bfloat16)


def prepare(tiled, starts, rows, pieces):
    steps = starts.shape[0] // pieces
    span = rows * LINES + 8

    def window(piece):
        return pl.BlockSpec(
            (pl.Element(span), pl.Element(GROUP)),
            lambda i, starts: (
                pl.multiple_of(starts[i * pieces + piece] // 8 * 8, 8),
                0,
            ),
        )

    return pl.pallas_call(
        functools.partial(prepare_kernel, pieces),
        grid_spec=pltpu.PrefetchScalarGridSpec(
            num_scalar_prefetch=1,
            grid=(steps,),
            in_specs=[window(piece) for piece in range(pieces)],
            out_specs=pl.BlockSpec(
                (LINES, pieces * rows, GROUP), lambda i, starts: (0, i, 0)
            ),
            scratch_shapes=[pltpu.VMEM(((rows + 1) * PITCH, GROUP), jnp.float32)],
        ),
        out_shape=jax.ShapeDtypeStruct(
            (LINES, steps * pieces * rows, GROUP), jnp.bfloat16
        ),
        cost_estimate=pl.CostEstimate(
            flops=4 * steps * pieces * span * GROUP,
            bytes_accessed=4 * steps * pieces * span * GROUP,
            transcendentals=0,
        ),
    )(starts, *[tiled] * pieces)


def rotate_kernel(base, place, tps, pads, window, *refs):
    outs, wide = refs[:-1], refs[-1]
    depth, rows = outs[0].shape[:2]
    pitch = wide.shape[0] // (rows + 1)
    tp = lax.axis_index("tp")
    shift = begin(base, place, pads) % 8
    for row in range(rows + 1):
        count = min(LINES, window.shape[0] - row * LINES)
        wide[pl.ds(row * pitch, count), :] = window[pl.ds(row * LINES, count), :].astype(
            jnp.float32
        )
    halves = len(outs) // tps
    for which, out in enumerate(outs):
        hop, half = which // halves, which % halves
        for line in range(depth):
            first = shift + ((tp + hop) % tps * halves + half) * depth + line
            first = jnp.where(first < LINES, first, first + pitch - LINES)
            picked = wide[pl.ds(first, rows, stride=pitch), :]
            out[line] = picked.astype(jnp.bfloat16)


def begin(base, place, pads):
    start = base
    for earlier in range(place):
        start = start + pads[earlier // len(WIDTHS), earlier % len(WIDTHS)]
    return start


def rotate(tiled, pads, base, place, rows, step, tps, halves):
    depth = LINES // tps // halves
    span = step * LINES + 8

    def window(i, pads):
        start = begin(base, place, pads) + i * step * LINES
        return (pl.multiple_of(start // 8 * 8, 8), 0)

    return pl.pallas_call(
        functools.partial(rotate_kernel, base, place, tps),
        grid_spec=pltpu.PrefetchScalarGridSpec(
            num_scalar_prefetch=1,
            grid=(rows // step,),
            in_specs=[pl.BlockSpec((pl.Element(span), pl.Element(GROUP)), window)],
            out_specs=[
                pl.BlockSpec((depth, step, GROUP), lambda i, pads: (0, i, 0))
            ]
            * tps
            * halves,
            scratch_shapes=[pltpu.VMEM(((step + 1) * PITCH, GROUP), jnp.float32)],
        ),
        out_shape=[jax.ShapeDtypeStruct((depth, rows, GROUP), jnp.bfloat16)]
        * tps
        * halves,
        cost_estimate=pl.CostEstimate(
            flops=4 * rows * D, bytes_accessed=4 * rows * D, transcendentals=0
        ),
    )(pads, tiled)


def exchange_kernel(reps, tps, sent, arrived, passing, send_a, recv_a, send_b, recv_b, kept):
    rep = lax.axis_index("rep")
    tp = lax.axis_index("tp")
    ratio = reps // tps
    depth = LINES // reps
    chunks = math.gcd(sent.shape[1] // 8, CHUNKS)
    rows = sent.shape[1] // chunks
    target = rep // ratio

    def at(device_rep, device_tp):
        return dict(
            device_id=(device_rep, device_tp), device_id_type=pl.DeviceIdType.MESH
        )

    barrier = pltpu.get_barrier_semaphore()
    for hop in range(1, reps):
        pl.semaphore_signal(barrier, inc=1, **at((rep + hop) % reps, tp))
    for hop in range(1, tps):
        pl.semaphore_signal(barrier, inc=1, **at(rep, (tp + hop) % tps))
    pl.semaphore_wait(barrier, reps + tps - 2)

    def block(chunk):
        return pl.ds(pl.multiple_of(chunk * rows, 8), rows)

    def mine(chunk, owner):
        return sent.at[pl.ds(owner * depth, depth), block(chunk)]

    def spread(chunk):
        for hop in range(1, reps):
            owner = (rep + hop) % reps

            def go(place):
                pltpu.make_async_remote_copy(
                    src_ref=mine(chunk, owner),
                    dst_ref=place,
                    send_sem=send_a.at[chunk],
                    recv_sem=recv_a.at[chunk],
                    **at(owner, tp),
                ).start()

            @pl.when(target == tp)
            def _():
                go(arrived.at[tp, rep % ratio, :, block(chunk)])

            @pl.when(target != tp)
            def _():
                go(passing.at[rep, :, block(chunk)])

    def forward(chunk):
        for hop in range(1, tps):
            there = (tp + hop) % tps
            for part in range(ratio):
                source = there * ratio + part

                def go(data):
                    pltpu.make_async_remote_copy(
                        src_ref=data,
                        dst_ref=arrived.at[tp, part, :, block(chunk)],
                        send_sem=send_b.at[chunk],
                        recv_sem=recv_b.at[chunk],
                        **at(rep, there),
                    ).start()

                @pl.when(source == rep)
                def _():
                    go(mine(chunk, rep))

                @pl.when(source != rep)
                def _():
                    go(passing.at[source, :, block(chunk)])

    @pl.when(target == tp)
    def _():
        pltpu.make_async_copy(
            sent.at[pl.ds(rep * depth, depth)], arrived.at[tp, rep % ratio], kept
        ).start()

    for chunk in range(AHEAD):
        spread(chunk)

    def wait(semaphore, chunk, count):
        whole = passing.at[pl.ds(0, count), :, block(chunk)]
        pltpu.make_async_copy(whole, whole, semaphore.at[chunk]).wait()

    @pl.loop(0, chunks)
    def _(chunk):
        @pl.when(chunk + AHEAD < chunks)
        def _():
            spread(chunk + AHEAD)

        wait(recv_a, chunk, reps - 1)
        forward(chunk)

    @pl.loop(0, chunks)
    def _(chunk):
        wait(send_a, chunk, reps - 1)
        wait(send_b, chunk, ratio * (tps - 1))
        wait(recv_b, chunk, ratio * (tps - 1))

    @pl.when(target == tp)
    def _():
        pltpu.make_async_copy(
            sent.at[pl.ds(rep * depth, depth)], arrived.at[tp, rep % ratio], kept
        ).wait()


def exchange(sent, reps, tps):
    rows = sent.shape[1]
    depth = LINES // reps
    size = 2 * sent.size
    arrived, _ = pl.pallas_call(
        functools.partial(exchange_kernel, reps, tps),
        in_specs=[pl.BlockSpec(memory_space=pl.ANY)],
        out_specs=[pl.BlockSpec(memory_space=pl.ANY)] * 2,
        out_shape=[
            jax.ShapeDtypeStruct((tps, reps // tps, depth, rows, GROUP), jnp.bfloat16),
            jax.ShapeDtypeStruct((reps, depth, rows, GROUP), jnp.bfloat16),
        ],
        scratch_shapes=[pltpu.SemaphoreType.DMA((CHUNKS,))] * 4
        + [pltpu.SemaphoreType.DMA],
        compiler_params=pltpu.CompilerParams(collective_id=0, has_side_effects=True),
        cost_estimate=pl.CostEstimate(
            flops=0, bytes_accessed=60 * size, transcendentals=0
        ),
    )(sent)
    return arrived


def columns(order, rows):
    width = math.gcd(rows, 256)
    chunks, chunk, size = [], [], 0
    for where in order:
        for begin in range(0, rows, width):
            chunk.append((where, begin, width))
            size += width
            if size % GROUP == 0 and size >= 256:
                chunks.append(chunk)
                chunk, size = [], 0
    return chunks + [chunk] if chunk else chunks


def settle(parts, scaled, group, column):
    part = parts[0] if len(parts) == 1 else jnp.concatenate(parts, axis=0)
    served = part.T.astype(jnp.float32)
    peak = jnp.max(jnp.abs(served), axis=0, keepdims=True) + 1e-06
    scaled[0, pl.ds(group * GROUP, GROUP), pl.ds(column, part.shape[0])] = (
        served * (1.0 / peak)
    ).astype(jnp.bfloat16)
    return peak


def quantize_kernel(chunks, *refs):
    tensors = len(refs) // 3
    for tensor, data in enumerate(refs[:tensors]):
        scaled, scale = refs[tensors + 2 * tensor :][:2]
        for group in range(scale.shape[0]):
            peaks, column = [], 0
            for chunk in chunks:
                parts = [
                    data[where + (group, pl.ds(begin, width))]
                    for where, begin, width in chunk
                ]
                peaks.append(settle(parts, scaled, group, column))
                column += peaks[-1].shape[1]
            peaks = jnp.concatenate(peaks, axis=1)
            for layer in range(LAYERS):

                @pl.when(pl.program_id(1) == layer)
                def _():
                    scale[group, pl.ds(layer, 1), :] = peaks


def finish_kernel(chunks, tps, layer, whole, *refs):
    received, scaled, scale = refs[:tps], refs[-2], refs[-1]
    batch = scale.shape[0]
    base = pl.program_id(0) * batch if whole else 0
    for before in range(layer):
        scale[:, before] = refs[-3][:, before]

    def run(mine):
        for group in range(batch):
            column = 0
            for chunk in chunks:
                parts = [
                    received[(mine - where) % tps][base + group, pl.ds(begin, width)]
                    for where, begin, width in chunk
                ]
                peak = settle(parts, scaled, group, column)
                scale[group, pl.ds(layer, 1), pl.ds(column, peak.shape[1])] = peak
                column += peak.shape[1]

    for mine in range(tps):
        pl.when(lax.axis_index("tp") == mine)(functools.partial(run, mine))


def finish(received, depth, batch, layer, half=0, earlier=()):
    tps = len(received)
    groups, rows = received[0].shape[:2]
    total = tps * rows
    skip = half * groups // batch
    whole = layer > 0
    if whole:
        source = pl.BlockSpec(memory_space=pltpu.VMEM)
    else:
        source = pl.BlockSpec((batch, rows, GROUP), lambda g: (g, 0, 0))
    scale = pl.BlockSpec((batch, LAYERS, total), lambda g: (skip + g, 0, 0))
    return pl.pallas_call(
        functools.partial(
            finish_kernel, columns(range(tps), rows), tps, layer, whole
        ),
        grid=(groups // batch,),
        in_specs=[source] * tps
        + [pl.BlockSpec(memory_space=pl.ANY), scale][: len(earlier)],
        out_specs=[
            pl.BlockSpec((1, batch * GROUP, total), lambda g: (layer, skip + g, 0)),
            scale,
        ],
        out_shape=[
            jax.ShapeDtypeStruct((LAYERS, depth * GROUP, total), jnp.bfloat16),
            jax.ShapeDtypeStruct((depth, LAYERS, total), jnp.float32),
        ],
        input_output_aliases={tps: 0, tps + 1: 1} if earlier else {},
        cost_estimate=pl.CostEstimate(
            flops=20 * groups * GROUP * total,
            bytes_accessed=4 * groups * GROUP * total,
            transcendentals=0,
        ),
    )(*received, *earlier)


def quantize(received, order, groups, rows, bases, batch):
    total = len(order) * rows
    lead = received.shape[:-3]
    zeros = (0,) * len(lead)

    def source(base):
        return pl.BlockSpec(
            lead + (batch, rows, GROUP), lambda g, l: zeros + (g, base + l, 0)
        )

    outputs = pl.pallas_call(
        functools.partial(quantize_kernel, columns(order, rows)),
        grid=(groups // batch, LAYERS),
        in_specs=[source(base) for base in bases],
        out_specs=[
            pl.BlockSpec((1, batch * GROUP, total), lambda g, l: (l, g, 0)),
            pl.BlockSpec((batch, LAYERS, total), lambda g, l: (g, 0, 0)),
        ]
        * len(bases),
        out_shape=[
            jax.ShapeDtypeStruct((LAYERS, groups * GROUP, total), jnp.bfloat16),
            jax.ShapeDtypeStruct((groups, LAYERS, total), jnp.float32),
        ]
        * len(bases),
        cost_estimate=pl.CostEstimate(
            flops=20 * len(bases) * LAYERS * groups * GROUP * total,
            bytes_accessed=4 * len(bases) * LAYERS * groups * GROUP * total,
            transcendentals=0,
        ),
    )(*[received] * len(bases))
    return [outputs[2 * i : 2 * i + 2] for i in range(len(bases))]


def on_device(flat_buffer, shard_pad):
    reps = lax.axis_size("rep")
    tps = lax.axis_size("tp")
    devices = reps * tps
    ratio = reps // tps
    rows = [width // devices for width in WIDTHS]
    tiled = flat_buffer.reshape(flat_buffer.shape[0] // GROUP, GROUP)
    bases = np.concatenate([[0], np.cumsum(rows * LAYERS)[:-1]]) * LINES
    pads = shard_pad.reshape(-1)

    def starts(tensors, step):
        base, before = [], []
        for index, layer in tensors:
            place = layer * len(WIDTHS) + index
            for row in range(0, rows[index], step):
                base.append(bases[place] + row * LINES)
                before.append(np.arange(pads.shape[0]) < place)
        before = jnp.asarray(np.array(before))
        shifts = jnp.sum(jnp.where(before, pads[None, :], 0), axis=1)
        return shifts + jnp.asarray(np.array(base, np.int32))

    wide = math.gcd(rows[3], FIRST)
    halves = math.gcd(LINES // tps, 2)
    sent_o = [
        rotate(
            tiled, shard_pad, int(bases[3 + layer * len(WIDTHS)]),
            3 + layer * len(WIDTHS), rows[3], wide, tps, halves if layer else 1,
        )
        for layer in range(LAYERS)
    ]

    def across(blocks):
        hops = sorted(range(1, tps), key=lambda hop: abs(2 * hop - tps))
        got = {
            hop: lax.ppermute(
                blocks[hop], "tp", [(at, (at + hop) % tps) for at in range(tps)]
            )
            for hop in hops
        }
        return [got.get(hop, blocks[0]) for hop in range(tps)]

    early = across(sent_o[0])
    step = math.gcd(*rows)
    sent = prepare(tiled, starts(ORDER, step), step, math.gcd(rows[4] // step, 4))
    sent, late = lax.optimization_barrier((sent, sent_o[1]))
    arrived = exchange(sent, reps, tps)
    arrived, late = lax.optimization_barrier((arrived, late))
    late = [across(late[half::halves]) for half in range(halves)]

    place, places = 0, {}
    for index in (0, 1, 2, 4, 5):
        places[index] = place // rows[index]
        place += LAYERS * rows[index]
    order = [(where, part) for part in range(ratio) for where in range(tps)]
    depth = LINES // reps
    outputs = [None] * len(WIDTHS)
    for batch, tensors in ((3, (4,)), (3, (5,)), (3, (0,)), (depth, (1, 2))):
        done = quantize(
            arrived,
            order,
            depth,
            rows[tensors[0]],
            [places[index] for index in tensors],
            math.gcd(batch, depth),
        )
        for index, pair in zip(tensors, done):
            outputs[index] = pair
    depth = LINES // tps
    batch = math.gcd(depth, 4)
    part = finish(early, depth, batch, 0)
    for half in range(halves):
        part = finish(late[half], depth, depth // halves, 1, half, tuple(part))
    outputs[3] = part
    return tuple(
        array for scaled, scale in outputs for array in (scaled, scale.transpose(1, 0, 2))
    )


def solution(mesh):
    column = P(None, "rep", "tp")
    row = P(None, "tp", "rep")
    return jax.shard_map(
        on_device,
        mesh=mesh,
        in_specs=(P(("rep", "tp")), P()),
        out_specs=(column,) * 6 + (row,) * 2 + (column,) * 4,
        check_vma=False,
    )
```
